32 devices in a mesh: row: 4 (over y, x), col: 8 (over z, core).
Axes of the slice: x: 2, y: 2, z: 4, core: 2. Of those that a mesh axis runs over, the one named last changes fastest.
Arguments:
- depth: float32 [256, 4096], P('row', 'col'), may hold values from 0 to 1
- rainfall: float32 [256, 4096], P('row', 'col'), may hold values from 0.05 to 0.5
- conveyance: float32 [256, 4096], P('row', 'col'), may hold values from 0.2 to 5
- flow_dir: int32 [256, 4096], P('row', 'col'), may hold values from 0 to 7, as said below
- outlet: int32 [256, 4096], P('row', 'col'), may hold values 0 or 1
Outputs:
- new_depth: float32 [256, 4096], P('row', 'col')
- discharge: float32 [256, 4096], P('row', 'col')
The draws below stay inside these ranges and needn't reach their ends.
Inputs may be any that keep to these rules, and one draw needn't show every extreme that they name: `flow_dir`: each cell's code is 0 to 7.
All inputs are finite; a program needn't handle non-finite values. No bound on the sum of `outlet` on one device may be relied on, other than what follows from the above.
Results may differ from the reference program's by a relative error of at most 0.00002.
Values sent between devices are 32-bit elements; how exact they have to be, the bound alone decides.
No kernel may reach another device: no remote copies, remote signals or barrier semaphores. Data moves between devices by JAX's collectives and lax.ppermute only.
A program may use at most 64 MiB of HBM per device.

```python
import math
import jax
import jax.numpy as jnp

SUBSTEPS = 3
PASSES = 64
NR = 256
NC = 4096


def draw_flow_dir(key, part):
    first = jax.random.fold_in(key, 11)
    second = jax.random.fold_in(key, 12)
    third = jax.random.fold_in(key, 13)
    picker = jax.random.randint(first, (NR, NC), 0, 10)
    drift = jax.random.randint(second, (NR, NC), 0, 3)
    anyway = jax.random.randint(third, (NR, NC), 0, 8)
    return jnp.where(picker < 7, drift, anyway).astype(jnp.int32)


def plant(array, key, low, top_value):
    longest = array.shape.index(max(array.shape))
    spots = []
    for shift in (0, 1):
        where = [jax.random.randint(jax.random.fold_in(key, axis), (), 0, length) for axis, length in enumerate(array.shape)]
        where[longest] = (where[longest] + shift) % array.shape[longest]
        spots.append(tuple(where))
    return array.at[spots[0]].set(low).at[spots[1]].set(top_value)


def levels(own_key, extent, split, low, largest):
    def one(axis_at, blocks):
        draws = jax.random.uniform(jax.random.fold_in(jax.random.fold_in(own_key, 6), axis_at), (blocks,), jnp.float32, low / len(split), largest / len(split))
        return jnp.repeat(jnp.exp(draws), extent[axis_at] // blocks).reshape((-1,) + (1,) * (len(extent) - axis_at - 1))

    gain = one(*split[0])
    for cut in split[1:]:
        gain = gain * one(*cut)
    return gain


def setup_inputs(seed: int = 0) -> dict:
    arg_keys = jax.random.split(jax.random.key(seed), 6)
    depth = jnp.clip(1.0 * jax.random.uniform(arg_keys[0], (NR, NC), jnp.float32) ** levels(arg_keys[0], (NR, NC), ((0, 4), (1, 8)), -0.2, 0.2), 0.0, 1.0)
    rainfall = jnp.clip(jnp.exp(math.log(0.5) - 2.3025851 * jax.random.uniform(arg_keys[1], (NR, NC), jnp.float32) ** levels(arg_keys[1], (NR, NC), ((0, 4), (1, 8)), -0.2, 0.2)), 0.05, 0.5)
    conveyance = jnp.clip(jnp.exp(math.log(5.0) - 3.218876 * jax.random.uniform(arg_keys[2], (NR, NC), jnp.float32) ** levels(arg_keys[2], (NR, NC), ((0, 4), (1, 8)), -0.2, 0.2)), 0.2, 5.0)
    flow_dir = draw_flow_dir(jax.random.fold_in(arg_keys[5], 71), 0)
    outlet = plant((jax.random.randint(arg_keys[4], (NR, NC), 0, 32) < 1).astype(jnp.int32), jax.random.fold_in(arg_keys[4], 1), 0, 1)
    return dict(depth=depth, rainfall=rainfall, conveyance=conveyance, flow_dir=flow_dir, outlet=outlet)


OFFSETS = ((0, 1), (1, 1), (1, 0), (1, -1), (0, -1), (-1, -1), (-1, 0), (-1, 1))


def inflow(sent, route):
    sent_pad = jnp.pad(sent, 1)
    route_pad = jnp.pad(route, 1)
    rows, cols = sent.shape
    total = jnp.zeros((rows, cols), jnp.float32)
    for k, (di, dj) in enumerate(OFFSETS):
        source = sent_pad[1 - di:1 - di + rows, 1 - dj:1 - dj + cols]
        target = route_pad[1 - di:1 - di + rows, 1 - dj:1 - dj + cols]
        total = total + jnp.where(target == k + 1, source, jnp.float32(0.0))
    return total


def reference(depth, rainfall, conveyance, flow_dir, outlet):
    route = jnp.where(outlet == 1, 0, flow_dir + 1).astype(jnp.int32)
    length = jnp.where(flow_dir % 2 == 1, jnp.float32(0.70710678), jnp.float32(1.0))
    level = depth
    for step in range(SUBSTEPS):
        factor = conveyance * length * jnp.power(level, jnp.float32(2.0 / 3.0))
        share = factor / (1.0 + factor)
        out = level * share
        sent = jnp.where(route > 0, out, jnp.float32(0.0))
        level = level + rainfall - out + inflow(sent, route)

    def one_pass(index, acc):
        sent = jnp.where(route > 0, acc, jnp.float32(0.0))
        return level + inflow(sent, route)

    acc = jax.lax.fori_loop(0, PASSES, one_pass, level)
    return level, jnp.log(1.0 + acc)
```

```python
import functools

import jax
import jax.numpy as jnp
from jax import lax
from jax.experimental import pallas as pl
from jax.experimental.pallas import tpu as pltpu
from jax.sharding import PartitionSpec as P

SUBSTEPS = 3
PASSES = 64


OFFSETS = ((0, 1), (1, 1), (1, 0), (1, -1), (0, -1), (-1, -1), (-1, 0), (-1, 1))


def extended(array, sides, width):
    for axis, dim in sides:
        peers, length = (lax.axis_size(axis), array.shape[dim])
        up = [(i, (i + 1) % peers) for i in range(peers - 1)]
        down = [(j, i) for i, j in up]
        last = lax.slice_in_dim(array, length - width, length, axis=dim)
        initial = lax.slice_in_dim(array, 0, width, axis=dim)
        before = lax.ppermute(last, axis, up)
        after = lax.ppermute(initial, axis, down)
        array = jnp.concatenate([before, array, after], axis=dim)
    return array


def padded_inflow(sent_pad, route_pad):
    rows = sent_pad.shape[0] - 2
    cols = sent_pad.shape[1] - 2
    total = jnp.zeros((rows, cols), jnp.float32)
    for k, (di, dj) in enumerate(OFFSETS):
        source = sent_pad[1 - di : 1 - di + rows, 1 - dj : 1 - dj + cols]
        target = route_pad[1 - di : 1 - di + rows, 1 - dj : 1 - dj + cols]
        total = total + jnp.where(target == k + 1, source, jnp.float32(0.0))
    return total


def on_device_tiles(depth, rainfall, conveyance, flow_dir, outlet):
    route = jnp.where(outlet == 1, 0, flow_dir + 1)
    length = jnp.where(flow_dir % 2 == 1, jnp.float32(0.70710678), jnp.float32(1.0))
    route_pad = extended(route, (("row", 0), ("col", 1)), 1)
    level = depth
    for step in range(SUBSTEPS):
        factor = conveyance * length * jnp.power(level, jnp.float32(2.0 / 3.0))
        share = factor / (1.0 + factor)
        out = level * share
        sent = jnp.where(route > 0, out, jnp.float32(0.0))
        sent_pad = extended(sent, (("row", 0), ("col", 1)), 1)
        level = level + rainfall - out + padded_inflow(sent_pad, route_pad)
    margin = 8
    route_wide = extended(route, (("row", 0), ("col", 1)), margin)
    level_wide = extended(level, (("row", 0), ("col", 1)), margin)
    rows, cols = level.shape

    def group_pass(index, acc):
        current = extended(acc, (("row", 0), ("col", 1)), margin)
        for inner in range(margin):
            edge = margin - inner
            route_here = route_wide[
                margin - edge : margin + rows + edge, margin - edge : margin + cols + edge
            ]
            level_here = level_wide[
                margin - edge + 1 : margin + rows + edge - 1,
                margin - edge + 1 : margin + cols + edge - 1,
            ]
            sent = jnp.where(route_here > 0, current, jnp.float32(0.0))
            current = level_here + padded_inflow(sent, route_here)
        return current

    acc = lax.fori_loop(0, PASSES // margin, group_pass, level)
    return (level, jnp.log(1.0 + acc))


LANES = 128
HALF = LANES // 2
SUB = 8
FIELDS = 4
SPARE = LANES // FIELDS
UNROLL = 2


def lane_of():
    return lax.broadcasted_iota(jnp.int32, (SUB, LANES), 1)


def coded(conveyance, flow_dir, outlet):
    length = jnp.where((flow_dir & 1) == 1, jnp.float32(0.70710678), jnp.float32(1.0))
    route = jnp.where(outlet == 1, 0, flow_dir + 1).astype(jnp.float32)
    return conveyance * length, route


def edge_kernel(*refs):
    rows = refs[0].shape[0]
    for side in range(2):
        depth, rain, conv, code, outlet = (ref[...] for ref in refs[5 * side : 5 * side + 5])
        factor, route = coded(conv, code, outlet)
        out = refs[10 + side]
        for f, value in enumerate((depth, rain, factor, route)):
            out[pl.ds(f * rows, rows), :] = value


def pack_kernel(peers, flags, depth, rain, conv, code, outlet, before, after, out):
    rows = depth.shape[0]
    lane = lax.broadcasted_iota(jnp.int32, (rows, LANES), 1)
    left = flags[0].astype(jnp.float32)
    right = flags[1].astype(jnp.float32)
    tiles = []
    first = [before[pl.ds(f * rows, rows), :] for f in range(FIELDS)]
    first[3] = first[3] * left
    tiles.append(first)
    for q in range(peers):
        cut = pl.ds(q * LANES, LANES)
        factor, route = coded(conv[:, cut], code[:, cut], outlet[:, cut])
        tiles.append([depth[:, cut], rain[:, cut], factor, route])
    last = [after[pl.ds(f * rows, rows), :] for f in range(FIELDS)]
    last[3] = last[3] * right
    tiles.append(last)
    for q in range(peers):
        spare = None
        for f in range(FIELDS):
            prev, own, following = tiles[q][f], tiles[q + 1][f], tiles[q + 2][f]
            out[q, pl.ds(2 * f * rows, rows), :] = own
            out[q, pl.ds((2 * f + 1) * rows, rows), :] = jnp.where(lane < HALF, following, prev)
            third = jnp.where(lane < HALF, prev, following)
            moved = pltpu.roll(third, (SPARE * f - HALF + SPARE // 2) % LANES, 1)
            spare = moved if spare is None else jnp.where(lane >= SPARE * f, moved, spare)
        out[q, pl.ds(2 * FIELDS * rows, rows), :] = spare


def shifted(tiles, lane, step):
    turned = [pltpu.roll(tile, step % LANES, 1) for tile in tiles]
    wrap = 0 if step == 1 else LANES - 1
    seam = HALF if step == 1 else HALF - 1
    own = jnp.where(lane == wrap, turned[1], turned[0])
    near = jnp.where(lane == wrap, turned[0], turned[1])
    if len(tiles) == 2:
        return [own, near]
    return [own, jnp.where(lane == seam, turned[2], near), jnp.where(lane == seam, turned[1], turned[2])]


def parts(masks, q, values, lane):
    count = len(values)
    east, west = shifted(values, lane, 1), shifted(values, lane, -1)
    here, down, above = [], [], []
    for t in range(count):
        v, e, w = values[t], east[t], west[t]
        m = [masks[k, q, t] for k in range(8)]
        here.append(m[0] * e + m[4] * w)
        down.append((m[1] * e + m[3] * w) + m[2] * v)
        above.append((m[7] * e + m[5] * w) + m[6] * v)
    return here, down, above


def sweep(masks, rows, count, lane, value, base, store):
    held = None
    for q in range(rows):
        here, down, above = parts(masks, q, value(q), lane)
        mine = [b + h for b, h in zip(base(q), here)]
        if q == 0:
            wrapped = [pltpu.roll(a, SUB - 1, 0) for a in above]
        else:
            done = [p + a for p, a in zip(pending, above)]
            if q == 1:
                held = done
            else:
                store(q - 1, done)
            mine = [p + d for p, d in zip(mine, carried)]
        pending, carried = mine, down
    store(rows - 1, [p + a for p, a in zip(pending, wrapped)])
    store(0, [p + pltpu.roll(d, 1, 0) for p, d in zip(held, carried)])


def strip_kernel(peers, got, out, flat, masks, rain, conv, level, total, final):
    block = got.shape[1] // (2 * FIELDS + 1)
    height = peers * block
    rows = height // SUB
    lane = lane_of()
    sub = lax.broadcasted_iota(jnp.int32, (SUB, LANES), 0)
    for p in range(peers):
        for f in range(2 * FIELDS + 1):
            flat[f, pl.ds(p * block, block), :] = got[p, pl.ds(f * block, block), :]

    def prepare(q, _):
        cut = pl.ds(q, SUB, stride=rows)
        spare = flat[2 * FIELDS, cut, :]
        field = []
        for f in range(FIELDS):
            third = pltpu.roll(spare, (HALF - SPARE // 2 - SPARE * f) % LANES, 1)
            field.append([flat[2 * f, cut, :], flat[2 * f + 1, cut, :], third])
        for t in range(3):
            level[q, t] = field[0][t]
            rain[q, t] = field[1][t]
            conv[q, t] = field[2][t]
        route = field[3]
        east, west = shifted(route, lane, 1), shifted(route, lane, -1)
        source = (east, east, route, west, west, west, route, east)
        top = jnp.logical_and(q == 0, sub == 0)
        bottom = jnp.logical_and(q == rows - 1, sub == SUB - 1)
        for k in range(8):
            di = OFFSETS[k][0]
            for t in range(3):
                hit = source[k][t] == jnp.float32(k + 1)
                if di == 1:
                    hit = jnp.logical_and(hit, jnp.logical_not(bottom))
                if di == -1:
                    hit = jnp.logical_and(hit, jnp.logical_not(top))
                masks[k, q, t] = jnp.where(hit, jnp.float32(1.0), jnp.float32(0.0))
        return 0

    lax.fori_loop(0, rows, prepare, 0)

    def substep(_, carry):
        def leaving(q, _):
            for t in range(3):
                h = level[q, t]
                a = conv[q, t] * jnp.exp(jnp.float32(2.0 / 3.0) * jnp.log(h))
                o = h * (a / (1.0 + a))
                total[q, t] = o
                level[q, t] = h + rain[q, t] - o
            return 0

        lax.fori_loop(0, rows, leaving, 0, unroll=2)

        def store(q, tiles):
            for t in range(3):
                level[q, t] = tiles[t]

        sweep(masks, rows, 3, lane, lambda q: [total[q, t] for t in range(3)], lambda q: [level[q, t] for t in range(3)], store)
        return carry

    lax.fori_loop(0, SUBSTEPS, substep, 0)

    def begin(q, _):
        for t in range(2):
            total[q, t] = level[q, t]
        final[0, pl.ds(q, SUB, stride=rows), :] = level[q, 0]
        return 0

    lax.fori_loop(0, rows, begin, 0, unroll=2)

    def store(q, tiles):
        for t in range(2):
            total[q, t] = tiles[t]

    def several(_, carry):
        for _ in range(UNROLL):
            sweep(masks, rows, 2, lane, lambda q: [total[q, t] for t in range(2)], lambda q: [level[q, t] for t in range(2)], store)
        return carry

    lax.fori_loop(0, PASSES // UNROLL, several, 0)

    def finish(q, _):
        final[1, pl.ds(q, SUB, stride=rows), :] = jnp.log(1.0 + total[q, 0])
        return 0

    lax.fori_loop(0, rows, finish, 0, unroll=2)
    for p in range(peers):
        for f in range(2):
            out[p, pl.ds(f * block, block), :] = final[f, pl.ds(p * block, block), :]


def join_kernel(peers, got, depth, discharge):
    rows = depth.shape[0]
    for q in range(peers):
        depth[:, pl.ds(q * LANES, LANES)] = got[q, pl.ds(0, rows), :]
        discharge[:, pl.ds(q * LANES, LANES)] = got[q, pl.ds(rows, rows), :]


def on_device_strips(depth, rainfall, conveyance, flow_dir, outlet):
    args = (depth, rainfall, conveyance, flow_dir, outlet)
    rows, cols = depth.shape
    peers, across = lax.axis_size("row"), lax.axis_size("col")
    place = lax.axis_index("col")
    vmem = pl.BlockSpec(memory_space=pltpu.VMEM)
    f32 = jnp.float32
    first = pl.BlockSpec((rows, LANES), lambda i: (0, 0))
    last = pl.BlockSpec((rows, LANES), lambda i: (0, cols // LANES - 1))
    edge = jax.ShapeDtypeStruct((FIELDS * rows, LANES), f32)
    low, high = pl.pallas_call(
        edge_kernel,
        grid=(1,),
        in_specs=[first] * 5 + [last] * 5,
        out_specs=[pl.BlockSpec((FIELDS * rows, LANES), lambda i: (0, 0))] * 2,
        out_shape=[edge, edge],
        name="edges",
    )(*args, *args)
    ring = [(i, (i + 1) % across) for i in range(across)]
    before = lax.ppermute(high, "col", ring)
    after = lax.ppermute(low, "col", [(j, i) for i, j in ring])
    flags = jnp.stack([place > 0, place < across - 1]).astype(jnp.int32)
    size = 2 * FIELDS + 1
    packed = pl.pallas_call(
        functools.partial(pack_kernel, peers),
        in_specs=[pl.BlockSpec(memory_space=pltpu.SMEM)] + [vmem] * 7,
        out_specs=vmem,
        out_shape=jax.ShapeDtypeStruct((peers, size * rows, LANES), f32),
        name="pack",
    )(flags, *args, before, after)
    got = lax.all_to_all(packed, "row", 0, 0, tiled=True)
    height = peers * rows
    tall = height // SUB
    made = pl.pallas_call(
        functools.partial(strip_kernel, peers),
        in_specs=[vmem],
        out_specs=vmem,
        out_shape=jax.ShapeDtypeStruct((peers, 2 * rows, LANES), f32),
        scratch_shapes=[
            pltpu.VMEM((size, height, LANES), f32),
            pltpu.VMEM((8, tall, 3, SUB, LANES), f32),
            pltpu.VMEM((tall, 3, SUB, LANES), f32),
            pltpu.VMEM((tall, 3, SUB, LANES), f32),
            pltpu.VMEM((tall, 3, SUB, LANES), f32),
            pltpu.VMEM((tall, 3, SUB, LANES), f32),
            pltpu.VMEM((2, height, LANES), f32),
        ],
        name="strip",
    )(got)
    back = lax.all_to_all(made, "row", 0, 0, tiled=True)
    whole = jax.ShapeDtypeStruct((rows, cols), f32)
    return pl.pallas_call(
        functools.partial(join_kernel, peers),
        in_specs=[vmem],
        out_specs=[vmem, vmem],
        out_shape=[whole, whole],
        name="join",
    )(back)


def on_device(*args):
    rows, cols = args[0].shape
    peers = lax.axis_size("row")
    fits = cols == peers * LANES and rows % SUB == 0 and PASSES <= HALF and SUBSTEPS <= SPARE // 2
    return tuple((on_device_strips if fits else on_device_tiles)(*args))


def solution(mesh):
    placed = (P("row", "col"), P("row", "col"), P("row", "col"), P("row", "col"), P("row", "col"))
    return jax.shard_map(
        on_device,
        mesh=mesh,
        in_specs=placed,
        out_specs=(P("row", "col"), P("row", "col")),
        check_vma=False,
    )
```

```python
import functools

import jax
import jax.numpy as jnp
from jax import lax
from jax.experimental import pallas as pl
from jax.experimental.pallas import tpu as pltpu
from jax.sharding import PartitionSpec as P

SUBSTEPS = 3
PASSES = 64


OFFSETS = ((0, 1), (1, 1), (1, 0), (1, -1), (0, -1), (-1, -1), (-1, 0), (-1, 1))


def extended(array, sides, width):
    for axis, dim in sides:
        peers, length = (lax.axis_size(axis), array.shape[dim])
        up = [(i, (i + 1) % peers) for i in range(peers - 1)]
        down = [(j, i) for i, j in up]
        last = lax.slice_in_dim(array, length - width, length, axis=dim)
        initial = lax.slice_in_dim(array, 0, width, axis=dim)
        before = lax.ppermute(last, axis, up)
        after = lax.ppermute(initial, axis, down)
        array = jnp.concatenate([before, array, after], axis=dim)
    return array


def padded_inflow(sent_pad, route_pad):
    rows = sent_pad.shape[0] - 2
    cols = sent_pad.shape[1] - 2
    total = jnp.zeros((rows, cols), jnp.float32)
    for k, (di, dj) in enumerate(OFFSETS):
        source = sent_pad[1 - di : 1 - di + rows, 1 - dj : 1 - dj + cols]
        target = route_pad[1 - di : 1 - di + rows, 1 - dj : 1 - dj + cols]
        total = total + jnp.where(target == k + 1, source, jnp.float32(0.0))
    return total


def on_device_tiles(depth, rainfall, conveyance, flow_dir, outlet):
    route = jnp.where(outlet == 1, 0, flow_dir + 1)
    length = jnp.where(flow_dir % 2 == 1, jnp.float32(0.70710678), jnp.float32(1.0))
    route_pad = extended(route, (("row", 0), ("col", 1)), 1)
    level = depth
    for step in range(SUBSTEPS):
        factor = conveyance * length * jnp.power(level, jnp.float32(2.0 / 3.0))
        share = factor / (1.0 + factor)
        out = level * share
        sent = jnp.where(route > 0, out, jnp.float32(0.0))
        sent_pad = extended(sent, (("row", 0), ("col", 1)), 1)
        level = level + rainfall - out + padded_inflow(sent_pad, route_pad)
    margin = 8
    route_wide = extended(route, (("row", 0), ("col", 1)), margin)
    level_wide = extended(level, (("row", 0), ("col", 1)), margin)
    rows, cols = level.shape

    def group_pass(index, acc):
        current = extended(acc, (("row", 0), ("col", 1)), margin)
        for inner in range(margin):
            edge = margin - inner
            route_here = route_wide[
                margin - edge : margin + rows + edge, margin - edge : margin + cols + edge
            ]
            level_here = level_wide[
                margin - edge + 1 : margin + rows + edge - 1,
                margin - edge + 1 : margin + cols + edge - 1,
            ]
            sent = jnp.where(route_here > 0, current, jnp.float32(0.0))
            current = level_here + padded_inflow(sent, route_here)
        return current

    acc = lax.fori_loop(0, PASSES // margin, group_pass, level)
    return (level, jnp.log(1.0 + acc))


LANES = 128
HALF = LANES // 2
SUB = 8
FIELDS = 4
SPARE = LANES // FIELDS
UNROLL = 2
PAD = SUB


def lane_of():
    return lax.broadcasted_iota(jnp.int32, (SUB, LANES), 1)


def coded(conveyance, flow_dir, outlet):
    length = jnp.where((flow_dir & 1) == 1, jnp.float32(0.70710678), jnp.float32(1.0))
    route = jnp.where(outlet == 1, 0, flow_dir + 1).astype(jnp.float32)
    return conveyance * length, route


def edge_kernel(*refs):
    rows = refs[0].shape[0]
    for side in range(2):
        depth, rain, conv, code, outlet = (ref[...] for ref in refs[5 * side : 5 * side + 5])
        factor, route = coded(conv, code, outlet)
        out = refs[10 + side]
        for f, value in enumerate((depth, rain, factor, route)):
            out[pl.ds(f * rows, rows), :] = value


def pack_kernel(peers, across, depth, rain, conv, code, outlet, before, after, out):
    rows = depth.shape[0]
    lane = lax.broadcasted_iota(jnp.int32, (rows, LANES), 1)
    place = lax.axis_index("col")
    left = jnp.where(place > 0, jnp.float32(1.0), jnp.float32(0.0))
    right = jnp.where(place < across - 1, jnp.float32(1.0), jnp.float32(0.0))
    tiles = []
    first = [before[pl.ds(f * rows, rows), :] for f in range(FIELDS)]
    first[3] = first[3] * left
    tiles.append(first)
    for q in range(peers):
        cut = pl.ds(q * LANES, LANES)
        factor, route = coded(conv[:, cut], code[:, cut], outlet[:, cut])
        tiles.append([depth[:, cut], rain[:, cut], factor, route])
    last = [after[pl.ds(f * rows, rows), :] for f in range(FIELDS)]
    last[3] = last[3] * right
    tiles.append(last)
    for q in range(peers):
        spare = None
        for f in range(FIELDS):
            prev, own, following = tiles[q][f], tiles[q + 1][f], tiles[q + 2][f]
            out[q, pl.ds(2 * f * rows, rows), :] = own
            out[q, pl.ds((2 * f + 1) * rows, rows), :] = jnp.where(lane < HALF, following, prev)
            third = jnp.where(lane < HALF, prev, following)
            moved = pltpu.roll(third, (SPARE * f - HALF + SPARE // 2) % LANES, 1)
            spare = moved if spare is None else jnp.where(lane >= SPARE * f, moved, spare)
        out[q, pl.ds(2 * FIELDS * rows, rows), :] = spare


def shifted(tiles, lane, step):
    turned = [pltpu.roll(tile, step % LANES, 1) for tile in tiles]
    wrap = 0 if step == 1 else LANES - 1
    seam = HALF if step == 1 else HALF - 1
    own = jnp.where(lane == wrap, turned[1], turned[0])
    near = jnp.where(lane == wrap, turned[0], turned[1])
    if len(tiles) == 2:
        return [own, near]
    return [own, jnp.where(lane == seam, turned[2], near), jnp.where(lane == seam, turned[1], turned[2])]


def parts(masks, q, values, lane):
    count = len(values)
    east, west = shifted(values, lane, 1), shifted(values, lane, -1)
    here, down, above = [], [], []
    for t in range(count):
        v, e, w = values[t], east[t], west[t]
        m = [masks[k, q, t] for k in range(8)]
        here.append(m[0] * e + m[4] * w)
        down.append((m[1] * e + m[3] * w) + m[2] * v)
        above.append((m[7] * e + m[5] * w) + m[6] * v)
    return here, down, above


def sweep(masks, rows, count, lane, value, base, store):
    held = None
    for q in range(rows):
        here, down, above = parts(masks, q, value(q), lane)
        mine = [b + h for b, h in zip(base(q), here)]
        if q == 0:
            wrapped = [pltpu.roll(a, SUB - 1, 0) for a in above]
        else:
            done = [p + a for p, a in zip(pending, above)]
            if q == 1:
                held = done
            else:
                store(q - 1, done)
            mine = [p + d for p, d in zip(mine, carried)]
        pending, carried = mine, down
    store(rows - 1, [p + a for p, a in zip(pending, wrapped)])
    store(0, [p + pltpu.roll(d, 1, 0) for p, d in zip(held, carried)])


def strip_kernel(peers, got, out, flat, masks, rain, conv, level, total, final):
    block = got.shape[1] // (2 * FIELDS + 1)
    height = peers * block
    rows = height // SUB
    lane = lane_of()
    sub = lax.broadcasted_iota(jnp.int32, (SUB, LANES), 0)
    pitch = rows + PAD
    share = SUB // peers
    for p in range(peers):
        for g in range(share):
            for f in range(2 * FIELDS + 1):
                flat[f, pl.ds((p * share + g) * pitch, rows), :] = got[p, pl.ds(f * block + g * rows, rows), :]

    def prepare(q, _):
        cut = pl.ds(q, SUB, stride=pitch)
        spare = flat[2 * FIELDS, cut, :]
        field = []
        for f in range(FIELDS):
            third = pltpu.roll(spare, (HALF - SPARE // 2 - SPARE * f) % LANES, 1)
            field.append([flat[2 * f, cut, :], flat[2 * f + 1, cut, :], third])
        for t in range(3):
            level[q, t] = field[0][t]
            rain[q, t] = field[1][t]
            conv[q, t] = field[2][t]
        route = field[3]
        east, west = shifted(route, lane, 1), shifted(route, lane, -1)
        source = (east, east, route, west, west, west, route, east)
        top = jnp.logical_and(q == 0, sub == 0)
        bottom = jnp.logical_and(q == rows - 1, sub == SUB - 1)
        for k in range(8):
            di = OFFSETS[k][0]
            for t in range(3):
                hit = source[k][t] == jnp.float32(k + 1)
                if di == 1:
                    hit = jnp.logical_and(hit, jnp.logical_not(bottom))
                if di == -1:
                    hit = jnp.logical_and(hit, jnp.logical_not(top))
                masks[k, q, t] = jnp.where(hit, jnp.float32(1.0), jnp.float32(0.0))
        return 0

    lax.fori_loop(0, rows, prepare, 0, unroll=8)

    def substep(_, carry):
        def leaving(q, _):
            for t in range(3):
                h = level[q, t]
                a = conv[q, t] * jnp.exp(jnp.float32(2.0 / 3.0) * jnp.log(h))
                o = h * (a / (1.0 + a))
                total[q, t] = o
                level[q, t] = h + rain[q, t] - o
            return 0

        lax.fori_loop(0, rows, leaving, 0, unroll=8)

        def store(q, tiles):
            for t in range(3):
                level[q, t] = tiles[t]

        sweep(masks, rows, 3, lane, lambda q: [total[q, t] for t in range(3)], lambda q: [level[q, t] for t in range(3)], store)
        return carry

    lax.fori_loop(0, SUBSTEPS, substep, 0)

    def begin(q, _):
        for t in range(2):
            total[q, t] = level[q, t]
        final[0, pl.ds(q, SUB, stride=pitch), :] = level[q, 0]
        return 0

    lax.fori_loop(0, rows, begin, 0, unroll=8)

    def store(q, tiles):
        for t in range(2):
            total[q, t] = tiles[t]

    def several(_, carry):
        for _ in range(UNROLL):
            sweep(masks, rows, 2, lane, lambda q: [total[q, t] for t in range(2)], lambda q: [level[q, t] for t in range(2)], store)
        return carry

    lax.fori_loop(0, PASSES // UNROLL, several, 0)

    def finish(q, _):
        final[1, pl.ds(q, SUB, stride=pitch), :] = jnp.log(1.0 + total[q, 0])
        return 0

    lax.fori_loop(0, rows, finish, 0, unroll=8)
    for p in range(peers):
        for g in range(share):
            for f in range(2):
                out[p, pl.ds(f * block + g * rows, rows), :] = final[f, pl.ds((p * share + g) * pitch, rows), :]


def join_kernel(peers, got, depth, discharge):
    rows = depth.shape[0]
    for q in range(peers):
        depth[:, pl.ds(q * LANES, LANES)] = got[q, pl.ds(0, rows), :]
        discharge[:, pl.ds(q * LANES, LANES)] = got[q, pl.ds(rows, rows), :]


def on_device_strips(depth, rainfall, conveyance, flow_dir, outlet):
    args = (depth, rainfall, conveyance, flow_dir, outlet)
    rows, cols = depth.shape
    peers, across = lax.axis_size("row"), lax.axis_size("col")
    vmem = pl.BlockSpec(memory_space=pltpu.VMEM)
    f32 = jnp.float32
    first = pl.BlockSpec((rows, LANES), lambda i: (0, 0))
    last = pl.BlockSpec((rows, LANES), lambda i: (0, cols // LANES - 1))
    edge = jax.ShapeDtypeStruct((FIELDS * rows, LANES), f32)
    low, high = pl.pallas_call(
        edge_kernel,
        grid=(1,),
        in_specs=[first] * 5 + [last] * 5,
        out_specs=[pl.BlockSpec((FIELDS * rows, LANES), lambda i: (0, 0))] * 2,
        out_shape=[edge, edge],
        name="edges",
    )(*args, *args)
    ring = [(i, (i + 1) % across) for i in range(across)]
    before = lax.ppermute(high, "col", ring)
    after = lax.ppermute(low, "col", [(j, i) for i, j in ring])
    size = 2 * FIELDS + 1
    packed = pl.pallas_call(
        functools.partial(pack_kernel, peers, across),
        in_specs=[vmem] * 7,
        out_specs=vmem,
        out_shape=jax.ShapeDtypeStruct((peers, size * rows, LANES), f32),
        name="pack",
    )(*args, before, after)
    got = lax.all_to_all(packed, "row", 0, 0, tiled=True)
    height = peers * rows
    tall = height // SUB
    made = pl.pallas_call(
        functools.partial(strip_kernel, peers),
        in_specs=[vmem],
        out_specs=vmem,
        out_shape=jax.ShapeDtypeStruct((peers, 2 * rows, LANES), f32),
        scratch_shapes=[
            pltpu.VMEM((size, height + SUB * PAD, LANES), f32),
            pltpu.VMEM((8, tall, 3, SUB, LANES), f32),
            pltpu.VMEM((tall, 3, SUB, LANES), f32),
            pltpu.VMEM((tall, 3, SUB, LANES), f32),
            pltpu.VMEM((tall, 3, SUB, LANES), f32),
            pltpu.VMEM((tall, 3, SUB, LANES), f32),
            pltpu.VMEM((2, height + SUB * PAD, LANES), f32),
        ],
        name="strip",
    )(got)
    back = lax.all_to_all(made, "row", 0, 0, tiled=True)
    whole = jax.ShapeDtypeStruct((rows, cols), f32)
    return pl.pallas_call(
        functools.partial(join_kernel, peers),
        in_specs=[vmem],
        out_specs=[vmem, vmem],
        out_shape=[whole, whole],
        name="join",
    )(back)


def on_device(*args):
    rows, cols = args[0].shape
    peers = lax.axis_size("row")
    fits = cols == peers * LANES and SUB % peers == 0 and (peers * rows) % (SUB * SUB) == 0 and PASSES <= HALF and SUBSTEPS <= SPARE // 2
    return tuple((on_device_strips if fits else on_device_tiles)(*args))


def solution(mesh):
    placed = (P("row", "col"), P("row", "col"), P("row", "col"), P("row", "col"), P("row", "col"))
    return jax.shard_map(
        on_device,
        mesh=mesh,
        in_specs=placed,
        out_specs=(P("row", "col"), P("row", "col")),
        check_vma=False,
    )
```

```python
import functools

import jax
import jax.numpy as jnp
from jax import lax
from jax.experimental import pallas as pl
from jax.experimental.pallas import tpu as pltpu
from jax.sharding import PartitionSpec as P

SUBSTEPS = 3
PASSES = 64


OFFSETS = ((0, 1), (1, 1), (1, 0), (1, -1), (0, -1), (-1, -1), (-1, 0), (-1, 1))


def extended(array, sides, width):
    for axis, dim in sides:
        peers, length = (lax.axis_size(axis), array.shape[dim])
        up = [(i, (i + 1) % peers) for i in range(peers - 1)]
        down = [(j, i) for i, j in up]
        last = lax.slice_in_dim(array, length - width, length, axis=dim)
        initial = lax.slice_in_dim(array, 0, width, axis=dim)
        before = lax.ppermute(last, axis, up)
        after = lax.ppermute(initial, axis, down)
        array = jnp.concatenate([before, array, after], axis=dim)
    return array


def padded_inflow(sent_pad, route_pad):
    rows = sent_pad.shape[0] - 2
    cols = sent_pad.shape[1] - 2
    total = jnp.zeros((rows, cols), jnp.float32)
    for k, (di, dj) in enumerate(OFFSETS):
        source = sent_pad[1 - di : 1 - di + rows, 1 - dj : 1 - dj + cols]
        target = route_pad[1 - di : 1 - di + rows, 1 - dj : 1 - dj + cols]
        total = total + jnp.where(target == k + 1, source, jnp.float32(0.0))
    return total


def on_device_tiles(depth, rainfall, conveyance, flow_dir, outlet):
    route = jnp.where(outlet == 1, 0, flow_dir + 1)
    length = jnp.where(flow_dir % 2 == 1, jnp.float32(0.70710678), jnp.float32(1.0))
    route_pad = extended(route, (("row", 0), ("col", 1)), 1)
    level = depth
    for step in range(SUBSTEPS):
        factor = conveyance * length * jnp.power(level, jnp.float32(2.0 / 3.0))
        share = factor / (1.0 + factor)
        out = level * share
        sent = jnp.where(route > 0, out, jnp.float32(0.0))
        sent_pad = extended(sent, (("row", 0), ("col", 1)), 1)
        level = level + rainfall - out + padded_inflow(sent_pad, route_pad)
    margin = 8
    route_wide = extended(route, (("row", 0), ("col", 1)), margin)
    level_wide = extended(level, (("row", 0), ("col", 1)), margin)
    rows, cols = level.shape

    def group_pass(index, acc):
        current = extended(acc, (("row", 0), ("col", 1)), margin)
        for inner in range(margin):
            edge = margin - inner
            route_here = route_wide[
                margin - edge : margin + rows + edge, margin - edge : margin + cols + edge
            ]
            level_here = level_wide[
                margin - edge + 1 : margin + rows + edge - 1,
                margin - edge + 1 : margin + cols + edge - 1,
            ]
            sent = jnp.where(route_here > 0, current, jnp.float32(0.0))
            current = level_here + padded_inflow(sent, route_here)
        return current

    acc = lax.fori_loop(0, PASSES // margin, group_pass, level)
    return (level, jnp.log(1.0 + acc))


LANES = 128
HALF = LANES // 2
SUB = 8
FIELDS = 4
UNROLL = 2
PAD = SUB


def sharing(peers):
    share = SUB // peers
    return share, LANES // (FIELDS * share)


def lane_of():
    return lax.broadcasted_iota(jnp.int32, (SUB, LANES), 1)


def coded(conveyance, flow_dir, outlet):
    length = jnp.where((flow_dir & 1) == 1, jnp.float32(0.70710678), jnp.float32(1.0))
    route = jnp.where(outlet == 1, 0, flow_dir + 1).astype(jnp.float32)
    return conveyance * length, route


def edge_kernel(*refs):
    rows = refs[0].shape[0]
    for side in range(2):
        depth, rain, conv, code, outlet = (ref[...] for ref in refs[5 * side : 5 * side + 5])
        factor, route = coded(conv, code, outlet)
        out = refs[10 + side]
        for f, value in enumerate((depth, rain, factor, route)):
            out[pl.ds(f * rows, rows), :] = value


def pack_kernel(peers, across, picks, *refs):
    depth, rain, conv, code, outlet = refs[:5]
    out, built, sems = refs[-3:]
    rows = depth.shape[0]
    lane = lax.broadcasted_iota(jnp.int32, (rows, LANES), 1)
    place = lax.axis_index("col")
    left = jnp.where(place > 0, jnp.float32(1.0), jnp.float32(0.0))
    right = jnp.where(place < across - 1, jnp.float32(1.0), jnp.float32(0.0))

    def tile(q):
        if q < 0 or q == peers:
            ref, inside = (refs[5], left) if q < 0 else (refs[6], right)
            fields = [ref[pl.ds(f * rows, rows), :] for f in range(FIELDS)]
            fields[3] = fields[3] * inside
            return fields
        cut = pl.ds(q * LANES, LANES)
        factor, route = coded(conv[:, cut], code[:, cut], outlet[:, cut])
        return [depth[:, cut], rain[:, cut], factor, route]

    share, width = sharing(peers)
    tall = rows // share
    copies = []
    for n, q in enumerate(picks):
        spare = None
        prevs, owns, followings = tile(q - 1), tile(q), tile(q + 1)
        for f in range(FIELDS):
            prev, own, following = prevs[f], owns[f], followings[f]
            built[n, pl.ds(2 * f * rows, rows), :] = own
            built[n, pl.ds((2 * f + 1) * rows, rows), :] = jnp.where(lane < HALF, following, prev)
            third = jnp.where(lane < HALF, prev, following)
            moved = pltpu.roll(third, (width * f - HALF + width // 2) % LANES, 1)
            spare = moved if spare is None else jnp.where(lane >= width * f, moved, spare)
        folded = spare[:tall]
        for g in range(1, share):
            group = pltpu.roll(spare[g * tall : (g + 1) * tall], g * FIELDS * width, 1)
            folded = jnp.where(lane[:tall] >= g * FIELDS * width, group, folded)
        built[n, pl.ds(2 * FIELDS * rows, tall), :] = folded
        copy = pltpu.make_async_copy(built.at[n], out.at[q], sems.at[n])
        copy.start()
        copies.append(copy)
    for copy in copies:
        copy.wait()


def shifted(tiles, lane, step):
    turned = [pltpu.roll(tile, step % LANES, 1) for tile in tiles]
    wrap = 0 if step == 1 else LANES - 1
    seam = HALF if step == 1 else HALF - 1
    own = jnp.where(lane == wrap, turned[1], turned[0])
    near = jnp.where(lane == wrap, turned[0], turned[1])
    if len(tiles) == 2:
        return [own, near]
    return [own, jnp.where(lane == seam, turned[2], near), jnp.where(lane == seam, turned[1], turned[2])]


def parts(masks, q, values, lane):
    count = len(values)
    east, west = shifted(values, lane, 1), shifted(values, lane, -1)
    here, down, above = [], [], []
    for t in range(count):
        v, e, w = values[t], east[t], west[t]
        m = [masks[k, q, t] for k in range(8)]
        here.append(m[0] * e + m[4] * w)
        down.append((m[1] * e + m[3] * w) + m[2] * v)
        above.append((m[7] * e + m[5] * w) + m[6] * v)
    return here, down, above


def sweep(masks, rows, count, lane, value, base, store):
    held = None
    for q in range(rows):
        here, down, above = parts(masks, q, value(q), lane)
        mine = [b + h for b, h in zip(base(q), here)]
        if q == 0:
            wrapped = [pltpu.roll(a, SUB - 1, 0) for a in above]
        else:
            done = [p + a for p, a in zip(pending, above)]
            if q == 1:
                held = done
            else:
                store(q - 1, done)
            mine = [p + d for p, d in zip(mine, carried)]
        pending, carried = mine, down
    store(rows - 1, [p + a for p, a in zip(pending, wrapped)])
    store(0, [p + pltpu.roll(d, 1, 0) for p, d in zip(held, carried)])


def strip_kernel(peers, got, out, flat, masks, rain, conv, level, total, final):
    share, width = sharing(peers)
    block = got.shape[1] * share // (2 * FIELDS * share + 1)
    height = peers * block
    rows = height // SUB
    lane = lane_of()
    sub = lax.broadcasted_iota(jnp.int32, (SUB, LANES), 0)
    pitch = rows + PAD
    for p in range(peers):
        for g in range(share):
            kept = got[p, pl.ds(2 * FIELDS * block, rows), :]
            if g:
                kept = pltpu.roll(kept, LANES - g * FIELDS * width, 1)
            flat[2 * FIELDS, pl.ds((p * share + g) * pitch, rows), :] = kept
            for f in range(2 * FIELDS):
                flat[f, pl.ds((p * share + g) * pitch, rows), :] = got[p, pl.ds(f * block + g * rows, rows), :]

    def prepare(q, _):
        cut = pl.ds(q, SUB, stride=pitch)
        spare = flat[2 * FIELDS, cut, :]
        field = []
        for f in range(FIELDS):
            third = pltpu.roll(spare, (HALF - width // 2 - width * f) % LANES, 1)
            field.append([flat[2 * f, cut, :], flat[2 * f + 1, cut, :], third])
        for t in range(3):
            level[q, t] = field[0][t]
            rain[q, t] = field[1][t]
            conv[q, t] = field[2][t]
        route = field[3]
        east, west = shifted(route, lane, 1), shifted(route, lane, -1)
        source = (east, east, route, west, west, west, route, east)
        top = jnp.logical_and(q == 0, sub == 0)
        bottom = jnp.logical_and(q == rows - 1, sub == SUB - 1)
        for k in range(8):
            di = OFFSETS[k][0]
            for t in range(3):
                hit = source[k][t] == jnp.float32(k + 1)
                if di == 1:
                    hit = jnp.logical_and(hit, jnp.logical_not(bottom))
                if di == -1:
                    hit = jnp.logical_and(hit, jnp.logical_not(top))
                masks[k, q, t] = jnp.where(hit, jnp.float32(1.0), jnp.float32(0.0))
        return 0

    lax.fori_loop(0, rows, prepare, 0, unroll=8)

    def substep(_, carry):
        def leaving(q, _):
            for t in range(3):
                h = level[q, t]
                a = conv[q, t] * jnp.exp(jnp.float32(2.0 / 3.0) * jnp.log(h))
                o = h * (a / (1.0 + a))
                total[q, t] = o
                level[q, t] = h + rain[q, t] - o
            return 0

        lax.fori_loop(0, rows, leaving, 0, unroll=8)

        def store(q, tiles):
            for t in range(3):
                level[q, t] = tiles[t]

        sweep(masks, rows, 3, lane, lambda q: [total[q, t] for t in range(3)], lambda q: [level[q, t] for t in range(3)], store)
        return carry

    lax.fori_loop(0, SUBSTEPS, substep, 0)

    def begin(q, _):
        for t in range(2):
            total[q, t] = level[q, t]
        final[0, pl.ds(q, SUB, stride=pitch), :] = level[q, 0]
        return 0

    lax.fori_loop(0, rows, begin, 0, unroll=8)

    def store(q, tiles):
        for t in range(2):
            total[q, t] = tiles[t]

    def several(_, carry):
        for _ in range(UNROLL):
            sweep(masks, rows, 2, lane, lambda q: [total[q, t] for t in range(2)], lambda q: [level[q, t] for t in range(2)], store)
        return carry

    lax.fori_loop(0, PASSES // UNROLL, several, 0)

    def finish(q, _):
        final[1, pl.ds(q, SUB, stride=pitch), :] = jnp.log(1.0 + total[q, 0])
        return 0

    lax.fori_loop(0, rows, finish, 0, unroll=8)
    for p in range(peers):
        for g in range(share):
            for f in range(2):
                out[p, pl.ds(f * block + g * rows, rows), :] = final[f, pl.ds((p * share + g) * pitch, rows), :]


def join_kernel(peers, got, depth, discharge):
    rows = depth.shape[0]
    for q in range(peers):
        depth[:, pl.ds(q * LANES, LANES)] = got[q, pl.ds(0, rows), :]
        discharge[:, pl.ds(q * LANES, LANES)] = got[q, pl.ds(rows, rows), :]


def on_device_strips(depth, rainfall, conveyance, flow_dir, outlet):
    args = (depth, rainfall, conveyance, flow_dir, outlet)
    rows, cols = depth.shape
    peers, across = lax.axis_size("row"), lax.axis_size("col")
    vmem = pl.BlockSpec(memory_space=pltpu.VMEM)
    f32 = jnp.float32
    first = pl.BlockSpec((rows, LANES), lambda i: (0, 0))
    last = pl.BlockSpec((rows, LANES), lambda i: (0, cols // LANES - 1))
    edge = jax.ShapeDtypeStruct((FIELDS * rows, LANES), f32)
    low, high = pl.pallas_call(
        edge_kernel,
        grid=(1,),
        in_specs=[first] * 5 + [last] * 5,
        out_specs=[pl.BlockSpec((FIELDS * rows, LANES), lambda i: (0, 0))] * 2,
        out_shape=[edge, edge],
        name="edges",
    )(*args, *args)
    ring = [(i, (i + 1) % across) for i in range(across)]
    before = lax.ppermute(high, "col", ring)
    after = lax.ppermute(low, "col", [(j, i) for i, j in ring])
    size = 2 * FIELDS + 1
    tallest = 2 * FIELDS * rows + rows // sharing(peers)[0]
    wide = jax.ShapeDtypeStruct((peers, tallest, LANES), f32)
    anywhere = pl.BlockSpec(memory_space=pl.ANY)

    def scratch(count):
        return [pltpu.VMEM((count, tallest, LANES), f32), pltpu.SemaphoreType.DMA((count,))]

    ends = sorted({0, peers - 1})
    inner = [q for q in range(peers) if q not in ends]
    operands, specs, alias = (*args, before, after), [vmem] * 7, {}
    if inner:
        partial = pl.pallas_call(
            functools.partial(pack_kernel, peers, across, inner),
            in_specs=[vmem] * 5,
            out_specs=anywhere,
            out_shape=wide,
            scratch_shapes=scratch(len(inner)),
            name="packinner",
        )(*args)
        operands, specs, alias = operands + (partial,), specs + [anywhere], {7: 0}
    packed = pl.pallas_call(
        functools.partial(pack_kernel, peers, across, ends),
        in_specs=specs,
        out_specs=anywhere,
        out_shape=wide,
        scratch_shapes=scratch(len(ends)),
        input_output_aliases=alias,
        name="packends",
    )(*operands)
    got = lax.all_to_all(packed, "row", 0, 0, tiled=True)
    height = peers * rows
    tall = height // SUB
    made = pl.pallas_call(
        functools.partial(strip_kernel, peers),
        in_specs=[vmem],
        out_specs=vmem,
        out_shape=jax.ShapeDtypeStruct((peers, 2 * rows, LANES), f32),
        scratch_shapes=[
            pltpu.VMEM((size, height + SUB * PAD, LANES), f32),
            pltpu.VMEM((8, tall, 3, SUB, LANES), f32),
            pltpu.VMEM((tall, 3, SUB, LANES), f32),
            pltpu.VMEM((tall, 3, SUB, LANES), f32),
            pltpu.VMEM((tall, 3, SUB, LANES), f32),
            pltpu.VMEM((tall, 3, SUB, LANES), f32),
            pltpu.VMEM((2, height + SUB * PAD, LANES), f32),
        ],
        name="strip",
    )(got)
    back = lax.all_to_all(made, "row", 0, 0, tiled=True)
    whole = jax.ShapeDtypeStruct((rows, cols), f32)
    return pl.pallas_call(
        functools.partial(join_kernel, peers),
        in_specs=[vmem],
        out_specs=[vmem, vmem],
        out_shape=[whole, whole],
        name="join",
    )(back)


def on_device(*args):
    rows, cols = args[0].shape
    peers = lax.axis_size("row")
    fits = cols == peers * LANES and SUB % peers == 0 and rows * peers % (SUB * SUB) == 0 and PASSES <= HALF and SUBSTEPS <= sharing(peers)[1] // 2
    return tuple((on_device_strips if fits else on_device_tiles)(*args))


def solution(mesh):
    placed = (P("row", "col"), P("row", "col"), P("row", "col"), P("row", "col"), P("row", "col"))
    return jax.shard_map(
        on_device,
        mesh=mesh,
        in_specs=placed,
        out_specs=(P("row", "col"), P("row", "col")),
        check_vma=False,
    )
```
